32 devices in a mesh: section: 2 (over x), dp: 16 (over z, y, core).
Axes of the slice: x: 2, y: 2, z: 4, core: 2. Of those that a mesh axis runs over, the one named last changes fastest.
Arguments:
- activations: bfloat16 [4, 256, 4608], P('section', 'dp'), may hold values from -6 to 6
- section_sources: int32 [4], replicated, may hold values from 0 to 3, as said below
- accumulators: float32 [256, 4, 4608], P('dp', 'section'), may hold values from -6 to 6
- block_sources: int32 [256], replicated, may hold values from 0 to 255, as said below
- loss_terms: float32 [2, 16], P('section', 'dp'), may hold values from 0.35 to 6
- pre_gain: float32 [2, 4608], P('section'), may hold values from 0.1 to 1.9
- query_weight: bfloat16 [2, 4608, 2048], P('section', None, 'dp'), may hold values from -0.09375 to 0.09375
- keyval_weight: bfloat16 [2, 4608, 2048], P('section', None, 'dp'), may hold values from -0.09375 to 0.09375
- output_weight: bfloat16 [2, 2048, 4608], P('section', 'dp'), may hold values from -0.125 to 0.125
- post_gain: float32 [2, 4608], P('section'), may hold values from 0.1 to 1.9
Outputs:
- new_activations: bfloat16 [4, 256, 4608], P('section', 'dp')
- new_accumulators: float32 [256, 4, 4608], P('dp', 'section')
- check_out: bfloat16 [2, 256, 4608], P('section', 'dp')
The draws below stay inside these ranges and needn't reach their ends.
Inputs may be any that keep to these rules, and one draw needn't show every extreme that they name: `section_sources`: A permutation; each old section's micro-batches fill 1 slots of each new section. `block_sources`: A permutation; each old data index's blocks fill 1 block of each new data index.
All inputs are finite; a program needn't handle non-finite values.
Results may differ from the reference program's by a relative error of at most 0.014.
Values may be sent and summed in bfloat16 or wider, within the bound.
No kernel may reach another device: no remote copies, remote signals or barrier semaphores. Data moves between devices by JAX's collectives and lax.ppermute only.
A program may use at most 64 MiB of HBM per device.

```python
import jax
import jax.numpy as jnp
from jax import lax

D = 4608
HD = 128
HEADS = 16
KV_HEADS = 8
TOKENS = 256
MB_DEV = 2
MB_ALL = 4
BROWS = 2
BLK_DEV = 16
BLOCKS = 256
ACC_ROWS = 4
N_SECTION = 2
N_DP = 16


def balanced_sources(key, groups, per_group):
    per_peer = per_group // groups

    def source_order(which):
        return jax.random.permutation(jax.random.fold_in(key, which), per_group)
    orders = jax.vmap(source_order)(jnp.arange(groups, dtype=jnp.int32))
    sources = jnp.arange(groups, dtype=jnp.int32)[:, None] * per_group + orders.astype(jnp.int32)
    chosen = sources.reshape(groups, groups, per_peer).transpose(1, 0, 2).reshape(groups, per_group)

    def shuffle(which, entries):
        return jax.random.permutation(jax.random.fold_in(key, 100000 + which), entries)
    table = jax.vmap(shuffle)(jnp.arange(groups, dtype=jnp.int32), chosen)
    return table.reshape(-1).astype(jnp.int32)


def draw_section_sources(key, part):
    return balanced_sources(jax.random.fold_in(key, 11), N_SECTION, MB_DEV)


def draw_block_sources(key, part):
    return balanced_sources(jax.random.fold_in(key, 23), N_DP, BLK_DEV)


def draw_loss_terms(key, part):
    rising = 1.0 + 2.0 * jnp.arange(N_DP, dtype=jnp.float32) / (N_DP - 1)
    subkey = jax.random.fold_in(key, 37)
    factor = jnp.exp(jax.random.uniform(subkey, (N_SECTION, N_DP), jnp.float32, jnp.log(0.7), jnp.log(1.4)))
    return (rising[None, :] * factor).astype(jnp.float32)


def shard_levels(stream_key, extent, shards, smallest, top_value):
    loudness, own = 1.0, jax.random.fold_in(stream_key, 6)
    for axis_at, blocks in shards:
        steps = jnp.exp(jax.random.uniform(jax.random.fold_in(own, axis_at), (blocks,), jnp.float32, smallest / len(shards), top_value / len(shards)))
        loudness = loudness * jnp.repeat(steps, extent[axis_at] // blocks).reshape([-1 if axis == axis_at else 1 for axis in range(len(extent))])
    return loudness


def bell_draw(rng, extent, spread, reach, shards=(), held_as=jnp.bfloat16):
    values = jax.random.normal(rng, extent, jnp.float32) * spread
    if len(shards) > 0:
        values = shard_levels(rng, extent, shards, -0.22, 0.18) * values
    return jnp.clip(values, min=-reach, max=reach).astype(held_as)


def setup_inputs(seed: int = 0) -> dict:
    seeds = jax.random.split(jax.random.key(seed), 11)
    activations = bell_draw(seeds[0], (MB_ALL, TOKENS, D), 1.0, 6.0, ((0, 2), (1, 16)))
    section_sources = draw_section_sources(jax.random.fold_in(seeds[10], 71), 0)
    accumulators = bell_draw(seeds[2], (BLOCKS, ACC_ROWS, D), 1.0, 6.0, ((0, 16), (1, 2)), jnp.float32)
    block_sources = draw_block_sources(jax.random.fold_in(seeds[10], 71), 0)
    loss_terms = draw_loss_terms(jax.random.fold_in(seeds[10], 71), 0)
    pre_gain = jnp.clip(1.0 + 0.18 * jax.random.normal(seeds[5], (N_SECTION, D), jnp.float32), 0.1, 1.9)
    query_weight = bell_draw(seeds[6], (N_SECTION, D, HEADS * HD), D ** -0.5, 0.09375, ((0, 2), (2, 16)))
    keyval_weight = bell_draw(seeds[7], (N_SECTION, D, HEADS * HD), D ** -0.5, 0.09375, ((0, 2), (2, 16)))
    output_weight = bell_draw(seeds[8], (N_SECTION, HEADS * HD, D), (HEADS * HD) ** -0.5, 0.125, ((0, 2), (1, 16)))
    post_gain = jnp.clip(1.0 + 0.18 * jax.random.normal(seeds[9], (N_SECTION, D), jnp.float32), 0.1, 1.9)
    return dict(activations=activations, section_sources=section_sources, accumulators=accumulators, block_sources=block_sources, loss_terms=loss_terms, pre_gain=pre_gain, query_weight=query_weight, keyval_weight=keyval_weight, output_weight=output_weight, post_gain=post_gain)


def rms_norm(values, gain):
    meansq = lax.optimization_barrier(jnp.mean(values * values, axis=-1, keepdims=True))
    return values * lax.rsqrt(meansq + 1e-06) * gain

def rotary(values, positions):
    width = values.shape[-1]
    middle = width // 2
    counter = jnp.arange(middle, dtype=jnp.float32)
    freqs = 10000.0 ** (-2.0 * counter / width)
    angles = positions.astype(jnp.float32)[:, None] * freqs[None, :]
    cosine = jnp.cos(angles)
    sine = jnp.sin(angles)
    if values.ndim == 3:
        cosine = cosine[:, None, :]
        sine = sine[:, None, :]
    first = values[..., :middle]
    second = values[..., middle:]
    return jnp.concatenate([first * cosine - second * sine, second * cosine + first * sine], axis=-1)

def check_layer(checked, gain_pre, w_query, w_keyval, w_output, gain_post):
    length = checked.shape[0]
    positions = jnp.arange(length, dtype=jnp.int32)
    normed = rms_norm(checked.astype(jnp.float32), gain_pre).astype(jnp.bfloat16)
    queries = jnp.dot(normed, w_query, preferred_element_type=jnp.float32).reshape(length, HEADS, HD)
    keyvals = jnp.dot(normed, w_keyval, preferred_element_type=jnp.float32).reshape(length, KV_HEADS, 2, HD)
    queries = rotary(queries, positions).astype(jnp.bfloat16)
    key_rows = rotary(keyvals[:, :, 0, :], positions).astype(jnp.bfloat16)
    value_rows = keyvals[:, :, 1, :].astype(jnp.bfloat16)
    key_rows = jnp.repeat(key_rows, 2, axis=1)
    value_rows = jnp.repeat(value_rows, 2, axis=1)
    scale_factor = (D / HEADS) ** (-0.5)
    scores = jnp.einsum('qhd,khd->hqk', queries.astype(jnp.float32), key_rows.astype(jnp.float32)) * scale_factor
    capped = 50.0 * jnp.tanh(scores / 50.0)
    causal = positions[None, :] <= positions[:, None]
    expd = jnp.where(causal[None, :, :], jnp.exp(capped), 0.0)
    denominator = lax.optimization_barrier(jnp.sum(expd, axis=-1))
    probs = expd.astype(jnp.bfloat16)
    numer = jnp.einsum('hqk,khd->hqd', probs.astype(jnp.float32), value_rows.astype(jnp.float32))
    attended = (numer / denominator[:, :, None]).astype(jnp.bfloat16)
    attended = jnp.transpose(attended, (1, 0, 2)).reshape(length, HEADS * HD)
    summed = jnp.dot(attended, w_output, preferred_element_type=jnp.float32)
    return (checked.astype(jnp.float32) + rms_norm(summed, gain_post)).astype(jnp.bfloat16)

def reference(activations, section_sources, accumulators, block_sources, loss_terms, pre_gain, query_weight, keyval_weight, output_weight, post_gain):
    moved = jnp.take(activations, section_sources, axis=0)
    regrouped = jnp.take(accumulators, block_sources, axis=0)
    totals = lax.optimization_barrier(jnp.sum(loss_terms, axis=1))
    factor = N_DP / totals
    scaled = regrouped.reshape(BLOCKS, N_SECTION, BROWS, D) * factor[None, :, None, None]
    new_accumulators = scaled.reshape(BLOCKS, ACC_ROWS, D)
    checks = []
    for section_id in range(N_SECTION):
        checks.append(check_layer(moved[section_id * MB_DEV], pre_gain[section_id], query_weight[section_id], keyval_weight[section_id], output_weight[section_id], post_gain[section_id]))
    return (moved, new_accumulators, jnp.stack(checks, axis=0))
```

```python
import jax
import jax.numpy as jnp
from jax import lax
from jax.sharding import PartitionSpec as P


def swap(value, axis, mask):
    pairs = [(source, source ^ mask) for source in range(lax.axis_size(axis))]
    return lax.ppermute(value, axis, pairs)


def rms_norm(values, gain):
    meansq = jnp.mean(values * values, axis=-1, keepdims=True)
    return values * lax.rsqrt(meansq + 1e-06) * gain


def rotary(values, positions):
    width = values.shape[-1]
    middle = width // 2
    counter = jnp.arange(middle, dtype=jnp.float32)
    freqs = 10000.0 ** (-2.0 * counter / width)
    angles = positions.astype(jnp.float32)[:, None] * freqs[None, :]
    cosine = jnp.cos(angles)
    sine = jnp.sin(angles)
    first = values[..., :middle]
    second = values[..., middle:]
    return jnp.concatenate(
        [first * cosine - second * sine, second * cosine + first * sine], axis=-1
    )


def routes(sources, own, groups):
    table = sources.reshape(groups, groups)
    owners = table // groups
    places = table % groups
    send = jnp.sum(jnp.where(owners == own, places, 0), axis=1)
    mine = lax.dynamic_slice_in_dim(owners, own, 1, 0)[0]
    return send, mine


def span(masks):
    order = [0]
    for mask in masks:
        order = order + [entry ^ mask for entry in order]
    return order


def on_device(
    activations,
    section_sources,
    accumulators,
    block_sources,
    loss_terms,
    pre_gain,
    query_weight,
    keyval_weight,
    output_weight,
    post_gain,
):
    sections = lax.axis_size("section")
    section = lax.axis_index("section")
    ranks = lax.axis_size("dp")
    rank = lax.axis_index("dp")
    tokens, width = activations.shape[1:]
    head = query_weight.shape[2]
    assert activations.shape[0] == sections and accumulators.shape[0] == ranks
    assert ranks & (ranks - 1) == 0 and sections & (sections - 1) == 0 and ranks >= 4

    mb_send, mb_from = routes(section_sources, section, sections)
    arrived = []
    for mask in range(sections):
        place = lax.dynamic_index_in_dim(mb_send, section ^ mask, 0, keepdims=False)
        item = lax.dynamic_index_in_dim(activations, place, 0, keepdims=False)
        arrived.append(item if mask == 0 else swap(item, "section", mask))

    def slot(j):
        value = arrived[0]
        for mask in range(1, sections):
            value = jnp.where(mb_from[j] == (section ^ mask), arrived[mask], value)
        return value

    checked = slot(0)
    moved = jnp.stack([checked] + [slot(j) for j in range(1, sections)])

    w_own = jnp.concatenate([query_weight[0], keyval_weight[0]], axis=1)
    wq_other = swap(query_weight[0], "dp", 1)
    wkv_other = swap(keyval_weight[0], "dp", 1)
    wo_other = swap(output_weight[0], "dp", 1)

    rest = [2**b for b in range(1, ranks.bit_length() - 1)]
    top = [rest[-1] | rest[-2]] if len(rest) > 1 else rest
    rest = rest[:-1] if len(rest) > 1 else []
    orders = [top + rest, top + rest[::-1]]
    normed = rms_norm(checked.astype(jnp.float32), pre_gain[0]).astype(jnp.bfloat16)
    cut = width // 256 * 128
    columns = [(0, cut), (cut, width)]
    layout = span(orders[0])
    parts = [normed[None, :, a:b] for a, b in columns]
    for step in range(len(orders[0])):
        sent = [swap(part, "dp", order[step]) for part, order in zip(parts, orders)]
        parts = [jnp.concatenate([part, got]) for part, got in zip(parts, sent)]
    rows = []
    for part, order in zip(parts, orders):
        have = span(order)
        if have != layout:
            part = jnp.concatenate([part[have.index(m)][None] for m in layout])
        rows.append(part.reshape(-1, part.shape[-1]))
    half = rows[0].shape[0]

    total = loss_terms
    for bit in range(ranks.bit_length() - 1):
        total = total + swap(total, "dp", 2**bit)
    factor = ranks / total[0, 0]
    block_send, block_from = routes(block_sources, rank, ranks)
    outgoing = jnp.take(accumulators, block_send, axis=0, mode="clip").astype(jnp.bfloat16)
    outgoing, rows = lax.optimization_barrier((outgoing, rows))
    incoming = lax.all_to_all(outgoing, "dp", split_axis=0, concat_axis=0, tiled=True)
    new_accumulators = (
        jnp.take(incoming, block_from, axis=0, mode="clip").astype(jnp.float32) * factor
    )

    weights = jnp.concatenate([w_own, wq_other, wkv_other], axis=1)
    proj = sum(
        jnp.dot(part, weights[a:b], preferred_element_type=jnp.float32)
        for part, (a, b) in zip(rows, columns)
    )
    own_at = (rank ^ jnp.array(layout, dtype=jnp.int32)) * tokens
    inner = jnp.arange(tokens, dtype=jnp.int32)
    positions = (own_at[:, None] + inner[None, :]).reshape(-1)
    other_at = (rank ^ jnp.array([m ^ 1 for m in layout], dtype=jnp.int32)) * tokens
    positions_other = (other_at[:, None] + inner[None, :]).reshape(-1)
    is_even = rank % 2 == 0
    q_own, kv_own, q_other, kv_other = (proj[:, i * head : (i + 1) * head] for i in range(4))
    keys = rotary(jnp.where(is_even, kv_own, kv_other), positions)
    values = jnp.where(is_even, kv_other, kv_own)
    keyval = jnp.concatenate([keys, values], axis=1).astype(jnp.bfloat16)
    keyval = jnp.concatenate([keyval, swap(keyval, "dp", 1)], axis=0)
    queries = jnp.concatenate(
        [rotary(q_own, positions), rotary(q_other, positions)], axis=0
    ).astype(jnp.bfloat16)

    key_at = jnp.concatenate([positions, positions_other])
    query_at = jnp.concatenate([positions, positions])
    scores = lax.dot_general(
        queries, keyval[:, :head], (((1,), (1,)), ((), ())), preferred_element_type=jnp.float32
    ) * ((width / ranks) ** (-0.5))
    capped = 50.0 * jnp.tanh(scores / 50.0)
    expd = jnp.where(key_at[None, :] <= query_at[:, None], jnp.exp(capped), 0.0)
    denominator = jnp.sum(expd, axis=-1, keepdims=True)
    numer = jnp.dot(
        expd.astype(jnp.bfloat16), keyval[:, head:], preferred_element_type=jnp.float32
    )
    attended = (numer / denominator).astype(jnp.bfloat16)
    attended = jnp.concatenate([attended[:half], attended[half:]], axis=1)
    w_out = jnp.concatenate([output_weight[0], wo_other], axis=0)

    sums = []
    for (a, b), order in zip(columns, orders):
        part = jnp.dot(attended, w_out[:, a:b], preferred_element_type=jnp.float32)
        part = part.reshape(-1, tokens, b - a)
        have = span(order)
        if have != layout:
            part = jnp.concatenate([part[layout.index(m)][None] for m in have])
        sums.append(part)
    for step in reversed(range(len(orders[0]))):
        sent = [
            swap(part[part.shape[0] // 2 :].astype(jnp.bfloat16), "dp", order[step])
            for part, order in zip(sums, orders)
        ]
        sums = [
            part[: part.shape[0] // 2] + got.astype(jnp.float32) for part, got in zip(sums, sent)
        ]
    summed = jnp.concatenate([part[0] for part in sums], axis=-1)
    check_out = (checked.astype(jnp.float32) + rms_norm(summed, post_gain[0])).astype(jnp.bfloat16)
    return (moved, new_accumulators, check_out[None, :, :])


def solution(mesh):
    placed = (
        P("section", "dp", None),
        P(),
        P("dp", "section", None),
        P(),
        P("section", "dp"),
        P("section", None),
        P("section", None, "dp"),
        P("section", None, "dp"),
        P("section", "dp", None),
        P("section", None),
    )
    return jax.shard_map(
        on_device,
        mesh=mesh,
        in_specs=placed,
        out_specs=(P("section", "dp", None), P("dp", "section", None), P("section", "dp", None)),
        check_vma=False,
    )
```

```python
import jax
import jax.numpy as jnp
from jax import lax
from jax.experimental import pallas as pl
from jax.experimental.pallas import tpu as pltpu
from jax.sharding import PartitionSpec as P


def swap(value, axis, mask):
    pairs = [(source, source ^ mask) for source in range(lax.axis_size(axis))]
    return lax.ppermute(value, axis, pairs)


def rms_norm(values, gain):
    meansq = jnp.mean(values * values, axis=-1, keepdims=True)
    return values * lax.rsqrt(meansq + 1e-06) * gain


def rotary(values, positions):
    width = values.shape[-1]
    middle = width // 2
    counter = jnp.arange(middle, dtype=jnp.float32)
    freqs = 10000.0 ** (-2.0 * counter / width)
    angles = positions.astype(jnp.float32)[:, None] * freqs[None, :]
    cosine = jnp.cos(angles)
    sine = jnp.sin(angles)
    first = values[..., :middle]
    second = values[..., middle:]
    return jnp.concatenate(
        [first * cosine - second * sine, second * cosine + first * sine], axis=-1
    )


def place_for(table, peer, own, groups):
    def look(j, place):
        entry = table[peer * groups + j]
        return place + jnp.where(entry // groups == own, entry % groups, 0)

    return lax.fori_loop(0, groups, look, jnp.int32(0), unroll=True)


def pick_sends(sources, section, items):
    groups = items.shape[0]

    def body(table, own_ref, held, out, sem):
        own = own_ref[0]
        copies = []
        for mask in range(1, groups):
            place = place_for(table, own ^ mask, own, groups)
            copies.append(pltpu.make_async_copy(held.at[place], out.at[mask - 1], sem.at[mask - 1]))
            copies[-1].start()
        for copy in copies:
            copy.wait()

    return pl.pallas_call(
        body,
        out_shape=jax.ShapeDtypeStruct((groups - 1,) + items.shape[1:], items.dtype),
        in_specs=[
            pl.BlockSpec(memory_space=pltpu.SMEM),
            pl.BlockSpec(memory_space=pltpu.SMEM),
            pl.BlockSpec(memory_space=pl.ANY),
        ],
        out_specs=pl.BlockSpec(memory_space=pltpu.VMEM),
        scratch_shapes=[pltpu.SemaphoreType.DMA((groups - 1,))],
        name="pick_sends",
    )(sources, section[None], items)


def pack_blocks(sources, rank, blocks, term):
    groups, rows, width = blocks.shape

    def body(table, own_ref, held, term_ref, out):
        own = own_ref[0]
        value = jnp.full((rows, 128), term_ref[0, 0], jnp.float32)
        coarse = value.astype(jnp.bfloat16)
        fine = (value - coarse.astype(jnp.float32)).astype(jnp.bfloat16)
        row = lax.broadcasted_iota(jnp.int32, (rows, 128), 0)
        tail = jnp.where(
            row == 0, coarse.astype(jnp.float32), jnp.where(row == 1, fine.astype(jnp.float32), 0.0)
        ).astype(jnp.bfloat16)

        def one(peer, carry):
            place = place_for(table, peer, own, groups)
            out[peer, :, :width] = held[place].astype(jnp.bfloat16)
            out[peer, :, width:] = tail
            return carry

        lax.fori_loop(0, groups, one, 0)

    return pl.pallas_call(
        body,
        out_shape=jax.ShapeDtypeStruct((groups, rows, width + 128), jnp.bfloat16),
        in_specs=[
            pl.BlockSpec(memory_space=pltpu.SMEM),
            pl.BlockSpec(memory_space=pltpu.SMEM),
            pl.BlockSpec(memory_space=pltpu.VMEM),
            pl.BlockSpec(memory_space=pltpu.SMEM),
        ],
        out_specs=pl.BlockSpec(memory_space=pltpu.VMEM),
        name="pack_blocks",
    )(sources, rank[None], blocks, term)


def place_blocks(sources, rank, blocks):
    groups, rows, width = blocks.shape
    width -= 128

    def body(table, own_ref, held, out):
        own = own_ref[0]

        def add(peer, total):
            return total + held[peer, :, width:].astype(jnp.float32)

        total = lax.fori_loop(0, groups, add, jnp.zeros((rows, 128), jnp.float32))
        factor = groups / jnp.sum(total, axis=0, keepdims=True)[:, :1]

        def one(slot, carry):
            owner = table[own * groups + slot] // groups
            out[slot] = held[owner, :, :width].astype(jnp.float32) * factor
            return carry

        lax.fori_loop(0, groups, one, 0)

    return pl.pallas_call(
        body,
        out_shape=jax.ShapeDtypeStruct((groups, rows, width), jnp.float32),
        in_specs=[
            pl.BlockSpec(memory_space=pltpu.SMEM),
            pl.BlockSpec(memory_space=pltpu.SMEM),
            pl.BlockSpec(memory_space=pltpu.VMEM),
        ],
        out_specs=pl.BlockSpec(memory_space=pltpu.VMEM),
        name="place_blocks",
    )(sources, rank[None], blocks)


def span(masks):
    order = [0]
    for mask in masks:
        order = order + [entry ^ mask for entry in order]
    return order


def step(
    activations,
    section_sources,
    accumulators,
    block_sources,
    loss_terms,
    pre_gain,
    query_weight,
    keyval_weight,
    output_weight,
    post_gain,
):
    sections = lax.axis_size("section")
    section = lax.axis_index("section")
    ranks = lax.axis_size("dp")
    rank = lax.axis_index("dp")
    tokens, width = activations.shape[1:]
    head = query_weight.shape[2]
    assert activations.shape[0] == sections and accumulators.shape[0] == ranks
    assert ranks & (ranks - 1) == 0 and sections & (sections - 1) == 0 and ranks >= 4

    sends = pick_sends(section_sources, section, activations)
    table = section_sources.reshape(sections, sections)
    mine = lax.dynamic_slice_in_dim(table, section, 1, 0)[0]
    mb_from = mine // sections
    kept = jnp.sum(jnp.where(mb_from == section, mine % sections, 0))
    arrived = [lax.dynamic_index_in_dim(activations, kept, 0, keepdims=False)]
    for mask in range(1, sections):
        arrived.append(swap(sends[mask - 1], "section", mask))
    outgoing = pack_blocks(block_sources, rank, accumulators, loss_terms)
    incoming = lax.all_to_all(outgoing, "dp", split_axis=0, concat_axis=0, tiled=True)

    def slot(j):
        value = arrived[0]
        for mask in range(1, sections):
            value = jnp.where(mb_from[j] == (section ^ mask), arrived[mask], value)
        return value

    checked = slot(0)
    moved = jnp.stack([checked] + [slot(j) for j in range(1, sections)])

    wq_other = swap(query_weight[0], "dp", 1)
    wkv_other = swap(keyval_weight[0], "dp", 1)
    wo_other = swap(output_weight[0], "dp", 1)
    weights = jnp.concatenate(
        [query_weight[0], keyval_weight[0], wq_other, wkv_other], axis=1
    )

    rest = [2**b for b in range(1, ranks.bit_length() - 1)]
    top = [rest[-1] | rest[-2]] if len(rest) > 1 else rest
    rest = rest[:-1] if len(rest) > 1 else []
    orders = [top + rest, top + rest[::-1]]
    normed = rms_norm(checked.astype(jnp.float32), pre_gain[0]).astype(jnp.bfloat16)
    cut = width // 256 * 128
    columns = [(0, cut), (cut, width)]
    layout = span(orders[0])
    parts = [normed[None, :, a:b] for a, b in columns]
    for stage in range(len(orders[0])):
        sent = [swap(part, "dp", order[stage]) for part, order in zip(parts, orders)]
        if stage == 1:
            weights, sent = lax.optimization_barrier((weights, sent))
        parts = [jnp.concatenate([part, got]) for part, got in zip(parts, sent)]
    rows = []
    for part, order in zip(parts, orders):
        have = span(order)
        if have != layout:
            part = jnp.concatenate([part[have.index(m)][None] for m in layout])
        rows.append(part.reshape(-1, part.shape[-1]))
    half = rows[0].shape[0]

    proj = sum(
        jnp.dot(part, weights[a:b], preferred_element_type=jnp.float32)
        for part, (a, b) in zip(rows, columns)
    )
    own_at = (rank ^ jnp.array(layout, dtype=jnp.int32)) * tokens
    inner = jnp.arange(tokens, dtype=jnp.int32)
    positions = (own_at[:, None] + inner[None, :]).reshape(-1)
    other_at = (rank ^ jnp.array([m ^ 1 for m in layout], dtype=jnp.int32)) * tokens
    positions_other = (other_at[:, None] + inner[None, :]).reshape(-1)
    is_even = rank % 2 == 0
    q_own, kv_own, q_other, kv_other = (proj[:, i * head : (i + 1) * head] for i in range(4))
    keys = rotary(jnp.where(is_even, kv_own, kv_other), positions)
    values = jnp.where(is_even, kv_other, kv_own)
    keyval = jnp.concatenate([keys, values], axis=1).astype(jnp.bfloat16)
    keyval = jnp.concatenate([keyval, swap(keyval, "dp", 1)], axis=0)
    queries = jnp.concatenate(
        [rotary(q_own, positions), rotary(q_other, positions)], axis=0
    ).astype(jnp.bfloat16)

    key_at = jnp.concatenate([positions, positions_other])
    query_at = jnp.concatenate([positions, positions])
    scores = lax.dot_general(
        queries, keyval[:, :head], (((1,), (1,)), ((), ())), preferred_element_type=jnp.float32
    ) * ((width / ranks) ** (-0.5))
    capped = 50.0 * jnp.tanh(scores / 50.0)
    expd = jnp.where(key_at[None, :] <= query_at[:, None], jnp.exp(capped), 0.0)
    denominator = jnp.sum(expd, axis=-1, keepdims=True)
    numer = jnp.dot(
        expd.astype(jnp.bfloat16), keyval[:, head:], preferred_element_type=jnp.float32
    )
    attended = (numer / denominator).astype(jnp.bfloat16)
    attended = jnp.concatenate([attended[:half], attended[half:]], axis=1)
    w_out = jnp.concatenate([output_weight[0], wo_other], axis=0)

    sums = []
    for (a, b), order in zip(columns, orders):
        part = jnp.dot(attended, w_out[:, a:b], preferred_element_type=jnp.float32)
        part = part.reshape(-1, tokens, b - a)
        have = span(order)
        if have != layout:
            part = jnp.concatenate([part[layout.index(m)][None] for m in have])
        sums.append(part)
    for stage in reversed(range(len(orders[0]))):
        sent = [
            swap(part[part.shape[0] // 2 :].astype(jnp.bfloat16), "dp", order[stage])
            for part, order in zip(sums, orders)
        ]
        if stage == len(orders[0]) - 1:
            incoming, sums = lax.optimization_barrier((incoming, sums))
            new_accumulators = place_blocks(block_sources, rank, incoming)
        sums = [
            part[: part.shape[0] // 2] + got.astype(jnp.float32) for part, got in zip(sums, sent)
        ]
    summed = jnp.concatenate([part[0] for part in sums], axis=-1)
    check_out = (checked.astype(jnp.float32) + rms_norm(summed, post_gain[0])).astype(jnp.bfloat16)
    return (moved, new_accumulators, check_out[None, :, :])


def solution(mesh):
    placed = (
        P("section", "dp", None),
        P(),
        P("dp", "section", None),
        P(),
        P("section", "dp"),
        P("section", None),
        P("section", None, "dp"),
        P("section", None, "dp"),
        P("section", "dp", None),
        P("section", None),
    )
    return jax.shard_map(
        step,
        mesh=mesh,
        in_specs=placed,
        out_specs=(P("section", "dp", None), P("dp", "section", None), P("section", "dp", None)),
        check_vma=False,
    )
```

```python
import jax
import jax.numpy as jnp
from jax import lax
from jax.experimental import pallas as pl
from jax.experimental.pallas import tpu as pltpu
from jax.sharding import PartitionSpec as P


def swap(value, axis, mask):
    pairs = [(source, source ^ mask) for source in range(lax.axis_size(axis))]
    return lax.ppermute(value, axis, pairs)


def rms_norm(values, gain):
    meansq = jnp.mean(values * values, axis=-1, keepdims=True)
    return values * lax.rsqrt(meansq + 1e-06) * gain


def rotary(values, positions):
    width = values.shape[-1]
    middle = width // 2
    counter = jnp.arange(middle, dtype=jnp.float32)
    freqs = 10000.0 ** (-2.0 * counter / width)
    angles = positions.astype(jnp.float32)[:, None] * freqs[None, :]
    cosine = jnp.cos(angles)
    sine = jnp.sin(angles)
    first = values[..., :middle]
    second = values[..., middle:]
    return jnp.concatenate(
        [first * cosine - second * sine, second * cosine + first * sine], axis=-1
    )


def place_for(table, peer, own, groups):
    shift = groups.bit_length() - 1

    def look(j, place):
        entry = table[peer * groups + j]
        return place + jnp.where(entry >> shift == own, entry & (groups - 1), 0)

    return lax.fori_loop(0, groups, look, jnp.int32(0), unroll=True)


def pick_sends(sources, section, items):
    groups = items.shape[0]

    def body(table, own_ref, held, out, sem):
        own = own_ref[0]
        copies = []
        for mask in range(1, groups):
            place = place_for(table, own ^ mask, own, groups)
            copies.append(pltpu.make_async_copy(held.at[place], out.at[mask - 1], sem.at[mask - 1]))
            copies[-1].start()
        for copy in copies:
            copy.wait()

    return pl.pallas_call(
        body,
        out_shape=jax.ShapeDtypeStruct((groups - 1,) + items.shape[1:], items.dtype),
        in_specs=[
            pl.BlockSpec(memory_space=pltpu.SMEM),
            pl.BlockSpec(memory_space=pltpu.SMEM),
            pl.BlockSpec(memory_space=pl.ANY),
        ],
        out_specs=pl.BlockSpec(memory_space=pl.ANY),
        scratch_shapes=[pltpu.SemaphoreType.DMA((groups - 1,))],
        compiler_params=pltpu.CompilerParams(vmem_limit_bytes=2**20),
        name="pick_sends",
    )(sources, section[None], items)


def pack_blocks(sources, rank, blocks, term):
    groups, rows, width = blocks.shape

    def body(table, own_ref, held, term_ref, out):
        own = own_ref[0]
        value = jnp.full((rows, 128), term_ref[0, 0], jnp.float32)
        coarse = value.astype(jnp.bfloat16)
        fine = (value - coarse.astype(jnp.float32)).astype(jnp.bfloat16)
        row = lax.broadcasted_iota(jnp.int32, (rows, 128), 0)
        tail = jnp.where(
            row == 0, coarse.astype(jnp.float32), jnp.where(row == 1, fine.astype(jnp.float32), 0.0)
        ).astype(jnp.bfloat16)

        def one(peer, carry):
            place = place_for(table, peer, own, groups)
            out[peer, :, :width] = held[place].astype(jnp.bfloat16)
            out[peer, :, width:] = tail
            return carry

        lax.fori_loop(0, groups, one, 0)

    return pl.pallas_call(
        body,
        out_shape=jax.ShapeDtypeStruct((groups, rows, width + 128), jnp.bfloat16),
        in_specs=[
            pl.BlockSpec(memory_space=pltpu.SMEM),
            pl.BlockSpec(memory_space=pltpu.SMEM),
            pl.BlockSpec(memory_space=pltpu.VMEM),
            pl.BlockSpec(memory_space=pltpu.SMEM),
        ],
        out_specs=pl.BlockSpec(memory_space=pltpu.VMEM),
        compiler_params=pltpu.CompilerParams(vmem_limit_bytes=2**20 + 4 * blocks.nbytes),
        name="pack_blocks",
    )(sources, rank[None], blocks, term)


def place_blocks(sources, rank, blocks):
    groups, rows, width = blocks.shape
    width -= 128

    def body(table, own_ref, held, out):
        own = own_ref[0]

        def add(peer, total):
            return total + held[peer, :, width:].astype(jnp.float32)

        total = lax.fori_loop(0, groups, add, jnp.zeros((rows, 128), jnp.float32))
        factor = groups / jnp.sum(total, axis=0, keepdims=True)[:, :1]

        def one(slot, carry):
            owner = table[own * groups + slot] >> (groups.bit_length() - 1)
            out[slot] = held[owner, :, :width].astype(jnp.float32) * factor
            return carry

        lax.fori_loop(0, groups, one, 0)

    return pl.pallas_call(
        body,
        out_shape=jax.ShapeDtypeStruct((groups, rows, width), jnp.float32),
        in_specs=[
            pl.BlockSpec(memory_space=pltpu.SMEM),
            pl.BlockSpec(memory_space=pltpu.SMEM),
            pl.BlockSpec(memory_space=pltpu.VMEM),
        ],
        out_specs=pl.BlockSpec(memory_space=pltpu.VMEM),
        compiler_params=pltpu.CompilerParams(vmem_limit_bytes=2**20 + 8 * blocks.nbytes),
        name="place_blocks",
    )(sources, rank[None], blocks)


def span(masks):
    order = [0]
    for mask in masks:
        order = order + [entry ^ mask for entry in order]
    return order


def turn(values, axes):
    bits = values.reshape((2,) * axes + (-1, values.shape[-1]))
    order = tuple(reversed(range(axes))) + (axes, axes + 1)
    return bits.transpose(order).reshape(values.shape)


def step(
    activations,
    section_sources,
    accumulators,
    block_sources,
    loss_terms,
    pre_gain,
    query_weight,
    keyval_weight,
    output_weight,
    post_gain,
):
    sections = lax.axis_size("section")
    section = lax.axis_index("section")
    ranks = lax.axis_size("dp")
    rank = lax.axis_index("dp")
    tokens, width = activations.shape[1:]
    head = query_weight.shape[2]
    assert activations.shape[0] == sections and accumulators.shape[0] == ranks
    assert ranks & (ranks - 1) == 0 and sections & (sections - 1) == 0 and ranks >= 4

    sends = pick_sends(section_sources, section, activations)
    table = section_sources.reshape(sections, sections)
    mine = lax.dynamic_slice_in_dim(table, section, 1, 0)[0]
    mb_from = mine // sections
    kept = jnp.sum(jnp.where(mb_from == section, mine % sections, 0))
    arrived = [lax.dynamic_index_in_dim(activations, kept, 0, keepdims=False)]
    for mask in range(1, sections):
        arrived.append(swap(sends[mask - 1], "section", mask))
    outgoing = pack_blocks(block_sources, rank, accumulators, loss_terms)
    incoming = lax.all_to_all(outgoing, "dp", split_axis=0, concat_axis=0, tiled=True)

    def slot(j):
        value = arrived[0]
        for mask in range(1, sections):
            value = jnp.where(mb_from[j] == (section ^ mask), arrived[mask], value)
        return value

    checked = slot(0)
    moved = jnp.stack([checked] + [slot(j) for j in range(1, sections)])

    wq_other = swap(query_weight[0], "dp", 1)
    wkv_other = swap(keyval_weight[0], "dp", 1)
    wo_other = swap(output_weight[0], "dp", 1)
    weights = jnp.concatenate(
        [query_weight[0], keyval_weight[0], wq_other, wkv_other], axis=1
    )

    rest = [2**b for b in range(1, ranks.bit_length() - 1)]
    top = [rest[-1] | rest[-2]] if len(rest) > 1 else rest
    rest = rest[:-1] if len(rest) > 1 else []
    orders = [top + rest, top + rest[::-1]]
    normed = rms_norm(checked.astype(jnp.float32), pre_gain[0]).astype(jnp.bfloat16)
    cut = width // 256 * 128
    columns = [(0, cut), (cut, width)]
    layout = span(orders[0])
    parts = [normed[None, :, a:b] for a, b in columns]
    for stage in range(len(orders[0])):
        sent = [swap(part, "dp", order[stage]) for part, order in zip(parts, orders)]
        if stage == 1:
            weights, sent = lax.optimization_barrier((weights, sent))
        parts = [jnp.concatenate([part, got]) for part, got in zip(parts, sent)]
    rows = [part.reshape(-1, part.shape[-1]) for part in parts]
    half = rows[0].shape[0]

    proj = [
        jnp.dot(part, weights[a:b], preferred_element_type=jnp.float32)
        for part, (a, b) in zip(rows, columns)
    ]
    proj = proj[0] + turn(proj[1], len(rest))
    own_at = (rank ^ jnp.array(layout, dtype=jnp.int32)) * tokens
    inner = jnp.arange(tokens, dtype=jnp.int32)
    positions = (own_at[:, None] + inner[None, :]).reshape(-1)
    other_at = (rank ^ jnp.array([m ^ 1 for m in layout], dtype=jnp.int32)) * tokens
    positions_other = (other_at[:, None] + inner[None, :]).reshape(-1)
    is_even = rank % 2 == 0
    q_own, kv_own, q_other, kv_other = (proj[:, i * head : (i + 1) * head] for i in range(4))
    keys = rotary(jnp.where(is_even, kv_own, kv_other), positions)
    values = jnp.where(is_even, kv_other, kv_own)
    keyval = jnp.concatenate([keys, values], axis=1).astype(jnp.bfloat16)
    keyval = jnp.concatenate([keyval, swap(keyval, "dp", 1)], axis=0)
    queries = jnp.concatenate(
        [rotary(q_own, positions), rotary(q_other, positions)], axis=0
    ).astype(jnp.bfloat16)

    key_at = jnp.concatenate([positions, positions_other])
    query_at = jnp.concatenate([positions, positions])
    scores = lax.dot_general(
        queries, keyval[:, :head], (((1,), (1,)), ((), ())), preferred_element_type=jnp.float32
    ) * ((width / ranks) ** (-0.5))
    capped = 50.0 * jnp.tanh(scores / 50.0)
    expd = jnp.where(key_at[None, :] <= query_at[:, None], jnp.exp(capped), 0.0)
    denominator = jnp.sum(expd, axis=-1, keepdims=True)
    numer = jnp.dot(
        expd.astype(jnp.bfloat16), keyval[:, head:], preferred_element_type=jnp.float32
    )
    attended = (numer / denominator).astype(jnp.bfloat16)
    attended = jnp.concatenate([attended[:half], attended[half:]], axis=1)
    w_out = jnp.concatenate([output_weight[0], wo_other], axis=0)

    sums = []
    for (a, b), source in zip(columns, [attended, turn(attended, len(rest))]):
        part = jnp.dot(source, w_out[:, a:b], preferred_element_type=jnp.float32)
        sums.append(part.reshape(-1, tokens, b - a))
    for stage in reversed(range(len(orders[0]))):
        sent = [
            swap(part[part.shape[0] // 2 :].astype(jnp.bfloat16), "dp", order[stage])
            for part, order in zip(sums, orders)
        ]
        sums = [
            part[: part.shape[0] // 2] + got.astype(jnp.float32) for part, got in zip(sums, sent)
        ]
    new_accumulators = place_blocks(block_sources, rank, incoming)
    summed = jnp.concatenate([part[0] for part in sums], axis=-1)
    check_out = (checked.astype(jnp.float32) + rms_norm(summed, post_gain[0])).astype(jnp.bfloat16)
    return (moved, new_accumulators, check_out[None, :, :])


def solution(mesh):
    placed = (
        P("section", "dp", None),
        P(),
        P("dp", "section", None),
        P(),
        P("section", "dp"),
        P("section", None),
        P("section", None, "dp"),
        P("section", None, "dp"),
        P("section", "dp", None),
        P("section", None),
    )
    return jax.shard_map(
        step,
        mesh=mesh,
        in_specs=placed,
        out_specs=(P("section", "dp", None), P("dp", "section", None), P("section", "dp", None)),
        check_vma=False,
    )
```

```python
import jax
import jax.numpy as jnp
from jax import lax
from jax.experimental import pallas as pl
from jax.experimental.pallas import tpu as pltpu
from jax.sharding import PartitionSpec as P


def swap(value, axis, mask):
    pairs = [(source, source ^ mask) for source in range(lax.axis_size(axis))]
    return lax.ppermute(value, axis, pairs)


def rms_norm(values, gain):
    meansq = jnp.mean(values * values, axis=-1, keepdims=True)
    return values * lax.rsqrt(meansq + 1e-06) * gain


def rotary(values, positions):
    width = values.shape[-1]
    middle = width // 2
    counter = jnp.arange(middle, dtype=jnp.float32)
    freqs = 10000.0 ** (-2.0 * counter / width)
    angles = positions.astype(jnp.float32)[:, None] * freqs[None, :]
    cosine = jnp.cos(angles)
    sine = jnp.sin(angles)
    first = values[..., :middle]
    second = values[..., middle:]
    return jnp.concatenate(
        [first * cosine - second * sine, second * cosine + first * sine], axis=-1
    )


def place_for(table, peer, own, groups):
    shift = groups.bit_length() - 1

    def look(j, place):
        entry = table[peer * groups + j]
        return place + jnp.where(entry >> shift == own, entry & (groups - 1), 0)

    return lax.fori_loop(0, groups, look, jnp.int32(0), unroll=True)


def pick_sends(sources, section, items):
    groups = items.shape[0]

    def body(table, own_ref, held, out, sem):
        own = own_ref[0]
        copies = []
        for mask in range(1, groups):
            place = place_for(table, own ^ mask, own, groups)
            copies.append(pltpu.make_async_copy(held.at[place], out.at[mask - 1], sem.at[mask - 1]))
            copies[-1].start()
        for copy in copies:
            copy.wait()

    return pl.pallas_call(
        body,
        out_shape=jax.ShapeDtypeStruct((groups - 1,) + items.shape[1:], items.dtype),
        in_specs=[
            pl.BlockSpec(memory_space=pltpu.SMEM),
            pl.BlockSpec(memory_space=pltpu.SMEM),
            pl.BlockSpec(memory_space=pl.ANY),
        ],
        out_specs=pl.BlockSpec(memory_space=pl.ANY),
        scratch_shapes=[pltpu.SemaphoreType.DMA((groups - 1,))],
        compiler_params=pltpu.CompilerParams(vmem_limit_bytes=2**20),
        name="pick_sends",
    )(sources, section[None], items)


def pack_blocks(sources, rank, blocks, term):
    groups, rows, width = blocks.shape

    def body(table, own_ref, held, term_ref, out):
        own = own_ref[0]
        value = jnp.full((rows, 128), term_ref[0, 0], jnp.float32)
        coarse = value.astype(jnp.bfloat16)
        fine = (value - coarse.astype(jnp.float32)).astype(jnp.bfloat16)
        row = lax.broadcasted_iota(jnp.int32, (rows, 128), 0)
        tail = jnp.where(
            row == 0, coarse.astype(jnp.float32), jnp.where(row == 1, fine.astype(jnp.float32), 0.0)
        ).astype(jnp.bfloat16)

        def one(peer, carry):
            place = place_for(table, peer, own, groups)
            out[peer, :, :width] = held[place].astype(jnp.bfloat16)
            out[peer, :, width:] = tail
            return carry

        lax.fori_loop(0, groups, one, 0)

    return pl.pallas_call(
        body,
        out_shape=jax.ShapeDtypeStruct((groups, rows, width + 128), jnp.bfloat16),
        in_specs=[
            pl.BlockSpec(memory_space=pltpu.SMEM),
            pl.BlockSpec(memory_space=pltpu.SMEM),
            pl.BlockSpec(memory_space=pltpu.VMEM),
            pl.BlockSpec(memory_space=pltpu.SMEM),
        ],
        out_specs=pl.BlockSpec(memory_space=pltpu.VMEM),
        compiler_params=pltpu.CompilerParams(vmem_limit_bytes=2**20 + 4 * blocks.nbytes),
        name="pack_blocks",
    )(sources, rank[None], blocks, term)


def place_blocks(sources, rank, blocks):
    groups, rows, width = blocks.shape
    width -= 128

    def body(table, own_ref, held, out):
        own = own_ref[0]

        def add(peer, total):
            return total + held[peer, :, width:].astype(jnp.float32)

        total = lax.fori_loop(0, groups, add, jnp.zeros((rows, 128), jnp.float32))
        factor = groups / jnp.sum(total, axis=0, keepdims=True)[:, :1]

        def one(slot, carry):
            owner = table[own * groups + slot] >> (groups.bit_length() - 1)
            out[slot] = held[owner, :, :width].astype(jnp.float32) * factor
            return carry

        lax.fori_loop(0, groups, one, 0)

    return pl.pallas_call(
        body,
        out_shape=jax.ShapeDtypeStruct((groups, rows, width), jnp.float32),
        in_specs=[
            pl.BlockSpec(memory_space=pltpu.SMEM),
            pl.BlockSpec(memory_space=pltpu.SMEM),
            pl.BlockSpec(memory_space=pltpu.VMEM),
        ],
        out_specs=pl.BlockSpec(memory_space=pltpu.VMEM),
        compiler_params=pltpu.CompilerParams(vmem_limit_bytes=2**20 + 8 * blocks.nbytes),
        name="place_blocks",
    )(sources, rank[None], blocks)


def span(masks):
    order = [0]
    for mask in masks:
        order = order + [entry ^ mask for entry in order]
    return order


def turn(values, axes):
    bits = values.reshape((2,) * axes + (-1, values.shape[-1]))
    order = tuple(reversed(range(axes))) + (axes, axes + 1)
    return bits.transpose(order).reshape(values.shape)


def step(
    activations,
    section_sources,
    accumulators,
    block_sources,
    loss_terms,
    pre_gain,
    query_weight,
    keyval_weight,
    output_weight,
    post_gain,
):
    sections = lax.axis_size("section")
    section = lax.axis_index("section")
    ranks = lax.axis_size("dp")
    rank = lax.axis_index("dp")
    tokens, width = activations.shape[1:]
    head = query_weight.shape[2]
    assert activations.shape[0] == sections and accumulators.shape[0] == ranks
    assert ranks & (ranks - 1) == 0 and sections & (sections - 1) == 0 and ranks >= 4

    sends = pick_sends(section_sources, section, activations)
    table = section_sources.reshape(sections, sections)
    mine = lax.dynamic_slice_in_dim(table, section, 1, 0)[0]
    mb_from = mine // sections
    kept = jnp.sum(jnp.where(mb_from == section, mine % sections, 0))
    arrived = [lax.dynamic_index_in_dim(activations, kept, 0, keepdims=False)]
    for mask in range(1, sections):
        arrived.append(swap(sends[mask - 1], "section", mask))
    outgoing = pack_blocks(block_sources, rank, accumulators, loss_terms)
    incoming = lax.all_to_all(outgoing, "dp", split_axis=0, concat_axis=0, tiled=True)

    def slot(j):
        value = arrived[0]
        for mask in range(1, sections):
            value = jnp.where(mb_from[j] == (section ^ mask), arrived[mask], value)
        return value

    checked = slot(0)
    moved = jnp.stack([checked] + [slot(j) for j in range(1, sections)])

    wq_other = swap(query_weight[0], "dp", 1)
    wkv_other = swap(keyval_weight[0], "dp", 1)
    wo_other = swap(output_weight[0], "dp", 1)
    weights = jnp.concatenate(
        [query_weight[0], keyval_weight[0], wq_other, wkv_other], axis=1
    )

    rest = [2**b for b in range(1, ranks.bit_length() - 1)]
    top = [rest[-1] | rest[-2]] if len(rest) > 1 else rest
    rest = rest[:-1] if len(rest) > 1 else []
    orders = [top + rest, top + rest[::-1]]
    normed = rms_norm(checked.astype(jnp.float32), pre_gain[0]).astype(jnp.bfloat16)
    late_rank, late_gain, normed = lax.optimization_barrier((rank, post_gain, normed))
    cut = width // 256 * 128
    columns = [(0, cut), (cut, width)]
    layout = span(orders[0])
    parts = [normed[None, :, a:b] for a, b in columns]
    for stage in range(len(orders[0])):
        sent = [swap(part, "dp", order[stage]) for part, order in zip(parts, orders)]
        parts = [jnp.concatenate([part, got]) for part, got in zip(parts, sent)]
    rows = [part.reshape(-1, part.shape[-1]) for part in parts]
    half = rows[0].shape[0]

    proj = [
        jnp.dot(part, weights[a:b], preferred_element_type=jnp.float32)
        for part, (a, b) in zip(rows, columns)
    ]
    proj = proj[0] + turn(proj[1], len(rest))
    own_at = (late_rank ^ jnp.array(layout, dtype=jnp.int32)) * tokens
    inner = jnp.arange(tokens, dtype=jnp.int32)
    positions = (own_at[:, None] + inner[None, :]).reshape(-1)
    other_at = (late_rank ^ jnp.array([m ^ 1 for m in layout], dtype=jnp.int32)) * tokens
    positions_other = (other_at[:, None] + inner[None, :]).reshape(-1)
    is_even = rank % 2 == 0
    q_own, kv_own, q_other, kv_other = (proj[:, i * head : (i + 1) * head] for i in range(4))
    keys = rotary(jnp.where(is_even, kv_own, kv_other), positions)
    values = jnp.where(is_even, kv_other, kv_own)
    keyval = jnp.concatenate([keys, values], axis=1).astype(jnp.bfloat16)
    keyval = jnp.concatenate([keyval, swap(keyval, "dp", 1)], axis=0)
    queries = jnp.concatenate(
        [rotary(q_own, positions), rotary(q_other, positions)], axis=0
    ).astype(jnp.bfloat16)

    key_at = jnp.concatenate([positions, positions_other])
    query_at = jnp.concatenate([positions, positions])
    scores = lax.dot_general(
        queries, keyval[:, :head], (((1,), (1,)), ((), ())), preferred_element_type=jnp.float32
    ) * ((width / ranks) ** (-0.5))
    capped = 50.0 * jnp.tanh(scores / 50.0)
    expd = jnp.where(key_at[None, :] <= query_at[:, None], jnp.exp(capped), 0.0)
    denominator = jnp.sum(expd, axis=-1, keepdims=True)
    numer = jnp.dot(
        expd.astype(jnp.bfloat16), keyval[:, head:], preferred_element_type=jnp.float32
    )
    attended = (numer / denominator).astype(jnp.bfloat16)
    attended = jnp.concatenate([attended[:half], attended[half:]], axis=1)
    w_out = jnp.concatenate([output_weight[0], wo_other], axis=0)

    sources = [attended, turn(attended, len(rest))]
    going, staying = [], []
    for (a, b), source in zip(columns, sources):
        part = jnp.dot(source[half // 2 :], w_out[:, a:b], preferred_element_type=jnp.float32)
        going.append(part.astype(jnp.bfloat16).reshape(-1, tokens, b - a))
    for (a, b), source in zip(columns, sources):
        part = jnp.dot(source[: half // 2], w_out[:, a:b], preferred_element_type=jnp.float32)
        staying.append(part.reshape(-1, tokens, b - a))
    for stage in reversed(range(len(orders[0]))):
        sent = [swap(part, "dp", order[stage]) for part, order in zip(going, orders)]
        middle = staying[0].shape[0] // 2
        if stage > 0:
            going = [
                (part[middle:] + got[middle:].astype(jnp.float32)).astype(jnp.bfloat16)
                for part, got in zip(staying, sent)
            ]
            staying = [
                part[:middle] + got[:middle].astype(jnp.float32)
                for part, got in zip(staying, sent)
            ]
        else:
            staying = [part + got.astype(jnp.float32) for part, got in zip(staying, sent)]
    sums = staying
    new_accumulators = place_blocks(block_sources, rank, incoming)
    summed = jnp.concatenate([part[0] for part in sums], axis=-1)
    check_out = (checked.astype(jnp.float32) + rms_norm(summed, late_gain[0])).astype(jnp.bfloat16)
    return (moved, new_accumulators, check_out[None, :, :])


def solution(mesh):
    placed = (
        P("section", "dp", None),
        P(),
        P("dp", "section", None),
        P(),
        P("section", "dp"),
        P("section", None),
        P("section", None, "dp"),
        P("section", None, "dp"),
        P("section", "dp", None),
        P("section", None),
    )
    return jax.shard_map(
        step,
        mesh=mesh,
        in_specs=placed,
        out_specs=(P("section", "dp", None), P("dp", "section", None), P("section", "dp", None)),
        check_vma=False,
    )
```
